128 devices in a mesh: ba: 16 (over y, x), ha: 8 (over z, core).
Axes of the slice: x: 4, y: 4, z: 4, core: 2. Of those that a mesh axis runs over, the one named last changes fastest.
Arguments:
- tokens: bfloat16 [128, 128, 4096], P(None, 'ba'), may hold values from -6 to 6
- w_query: bfloat16 [4096, 4096], P(None, 'ha'), may hold values from -0.09375 to 0.09375
- w_keyval: bfloat16 [4096, 512], P(None, 'ha'), may hold values from -0.09375 to 0.09375
- w_out: bfloat16 [4096, 4096], P('ha'), may hold values from -0.09375 to 0.09375
- cache_kv: bfloat16 [128, 2048, 512], P(('ba', 'ha')), may hold values from -1700 to 1700
- lengths: int32 [128], replicated, may hold values from 0 to 2048
- slot_seq: int32 [128], replicated, may hold values from 0 to 127, each once
Outputs:
- attended: bfloat16 [128, 128, 4096], P('ha', 'ba')
The draws below stay inside these ranges and needn't reach their ends.
Inputs may be any that keep to these rules, and one draw needn't show every extreme that they name: slot_seq names every sequence exactly once.
All inputs are finite; a program needn't handle non-finite values.
Results may differ from the reference program's by a relative error of at most 0.015.
The reference program's roundings to bfloat16 on the way (of `query`, `keyval`, `probs` and `heads_out`) count: a program that leaves them out, or rounds other values in their place, can miss the bound.
Values may be sent and summed in bfloat16 or wider, within the bound.
No kernel may reach another device: no remote copies, remote signals or barrier semaphores. Data moves between devices by JAX's collectives and lax.ppermute only.
A program may use at most 128 MiB of HBM per device.

```python
import jax
import jax.numpy as jnp
from jax import lax

D = 4096
HQ = 16
HD = 256
NEW = 128
PREFIX = 2048
SEQS = 128


def draw_cache_kv(key, part):
    base = jnp.clip(jax.random.normal(key, (SEQS, PREFIX, 2 * HD), jnp.float32), -6.0, 6.0)
    return base.astype(jnp.bfloat16)


def place_ends(result, stream_key, least, top_value):
    place = [jax.random.randint(jax.random.fold_in(stream_key, axis), (), 0, length) for axis, length in enumerate(result.shape)]
    main_axis = result.shape.index(max(result.shape))
    next_to = place[:main_axis] + [(place[main_axis] + 1) % result.shape[main_axis]] + place[main_axis + 1:]
    return result.at[tuple(place)].set(least).at[tuple(next_to)].set(top_value)


def steps_of(stream_key, shape, cuts, least, top_value):
    loudness, own = 1.0, jax.random.fold_in(stream_key, 6)
    for dim, blocks in cuts:
        draws = jnp.exp(jax.random.uniform(jax.random.fold_in(own, dim), (blocks,), jnp.float32, least / len(cuts), top_value / len(cuts)))
        loudness = loudness * jnp.repeat(draws, shape[dim] // blocks).reshape([-1 if axis == dim else 1 for axis in range(len(shape))])
    return loudness


def scatter_about(own_key, extent, width, most, cuts=(), kind=jnp.bfloat16):
    loudness = steps_of(own_key, extent, cuts, -0.22, 0.18) if cuts else 1.0
    values = jax.random.normal(own_key, extent, jnp.float32) * width * loudness
    return jnp.minimum(jnp.maximum(values, -most), most).astype(kind)


def setup_inputs(seed: int = 0) -> dict:
    arg_keys = jax.random.split(jax.random.key(seed), 8)
    tokens = scatter_about(arg_keys[0], (SEQS, NEW, D), 1.0, 6.0, ((1, 16),))
    w_query = scatter_about(arg_keys[1], (D, HQ * HD), D ** -0.5, 0.09375, ((1, 8),))
    w_keyval = scatter_about(arg_keys[2], (D, 2 * HD), D ** -0.5, 0.09375, ((1, 8),))
    w_out = scatter_about(arg_keys[3], (HQ * HD, D), (HQ * HD) ** -0.5, 0.09375, ((0, 8),))
    cache_kv = draw_cache_kv(jax.random.fold_in(arg_keys[7], 71), 0)
    lengths = place_ends(jax.random.randint(arg_keys[5], (SEQS,), 0, PREFIX + 1), jax.random.fold_in(arg_keys[5], 1), 0, PREFIX).astype(jnp.int32)
    slot_seq = jax.random.permutation(arg_keys[6], SEQS).astype(jnp.int32)
    return {"tokens": tokens, "w_query": w_query, "w_keyval": w_keyval, "w_out": w_out, "cache_kv": cache_kv, "lengths": lengths, "slot_seq": slot_seq}


def attend_slot(query, keyval, cache_kv, lengths, slot_seq, slot):
    seq = slot_seq[slot]
    q_seq = lax.dynamic_index_in_dim(query, seq, 0, keepdims=False)
    kv_seq = lax.dynamic_index_in_dim(keyval, seq, 0, keepdims=False)
    cache = lax.dynamic_index_in_dim(cache_kv, slot, 0, keepdims=False)
    live = lengths[seq]
    keys = jnp.concatenate([cache[:, :HD], kv_seq[:, :HD]], axis=0).astype(jnp.float32)
    values = jnp.concatenate([cache[:, HD:], kv_seq[:, HD:]], axis=0).astype(jnp.float32)
    scores = jnp.einsum('nhd,kd->hnk', q_seq.astype(jnp.float32), keys) / jnp.sqrt(jnp.float32(HD))
    position = jnp.arange(PREFIX + NEW, dtype=jnp.int32)[None, :]
    row = jnp.arange(NEW, dtype=jnp.int32)[:, None]
    allowed = jnp.where(position < PREFIX, position < live, position - PREFIX <= row)
    scores = jnp.where(allowed[None], scores, jnp.float32(-1e+30))
    probs = jax.nn.softmax(scores, axis=-1).astype(jnp.bfloat16)
    heads_out = jnp.einsum('hnk,kd->nhd', probs.astype(jnp.float32), values)
    return heads_out.reshape(NEW, HQ * HD).astype(jnp.bfloat16)

def reference(tokens, w_query, w_keyval, w_out, cache_kv, lengths, slot_seq):
    flat = tokens.reshape(SEQS * NEW, D)
    query = jnp.dot(flat, w_query, preferred_element_type=jnp.float32).astype(jnp.bfloat16).reshape(SEQS, NEW, HQ, HD)
    keyval = jnp.dot(flat, w_keyval, preferred_element_type=jnp.float32).astype(jnp.bfloat16).reshape(SEQS, NEW, 2 * HD)
    slots = jnp.arange(SEQS, dtype=jnp.int32)
    per_slot = lax.map(lambda slot: attend_slot(query, keyval, cache_kv, lengths, slot_seq, slot), slots)
    inverse = jnp.zeros((SEQS,), jnp.int32).at[slot_seq].set(slots)
    by_seq = jnp.take(per_slot, inverse, axis=0)
    attended = jnp.dot(by_seq.reshape(SEQS * NEW, HQ * HD), w_out, preferred_element_type=jnp.float32)
    return attended.astype(jnp.bfloat16).reshape(SEQS, NEW, D)
```

```python
import functools

import jax
import jax.numpy as jnp
from jax import lax
from jax.experimental import pallas as pl
from jax.experimental.pallas import tpu as pltpu
from jax.sharding import PartitionSpec as P

HD = 256
NEG = -1e30
F32 = jnp.float32
BF16 = jnp.bfloat16


VMEM_WHOLE = pl.BlockSpec(memory_space=pltpu.VMEM)


def in_hbm(x):
    return pltpu.with_memory_space_constraint(x, pltpu.HBM)


def project_kernel(slot_seq, tok, wq, wkv, out, accq, acckv):
    step = pl.program_id(0)
    seqs, tblock, depth = tok.shape
    x = tok[...].reshape(seqs * tblock, depth)
    q = jnp.dot(x, wq[...], preferred_element_type=F32)
    kv = lax.dot_general(x, wkv[...], (((1,), (1,)), ((), ())), preferred_element_type=F32)

    @pl.when(step == 0)
    def _():
        accq[...] = q
        acckv[...] = kv

    @pl.when(step > 0)
    def _():
        accq[...] += q
        acckv[...] += kv

    @pl.when(step == pl.num_programs(0) - 1)
    def _():
        cols = accq.shape[1]

        @pl.loop(0, seqs, unroll=8)
        def _(c):
            rows = pl.ds(slot_seq[c] * tblock, tblock)
            out[c, :, :cols] = accq[rows, :].astype(BF16)
            out[c, :, cols:] = acckv[rows, :].astype(BF16)


def project(tokens, w_query, w_keyval_t, slot_seq):
    seqs, tblock, width = tokens.shape
    cols, kvcols = w_query.shape[1], w_keyval_t.shape[0]
    depth = 512
    return pl.pallas_call(
        project_kernel,
        name="project",
        out_shape=jax.ShapeDtypeStruct((seqs, tblock, cols + kvcols), BF16),
        grid_spec=pltpu.PrefetchScalarGridSpec(
            num_scalar_prefetch=1,
            grid=(width // depth,),
            in_specs=[
                pl.BlockSpec((seqs, tblock, depth), lambda k, s: (0, 0, k)),
                pl.BlockSpec((depth, cols), lambda k, s: (k, 0)),
                pl.BlockSpec((kvcols, depth), lambda k, s: (0, k)),
            ],
            out_specs=pl.BlockSpec((seqs, tblock, cols + kvcols), lambda k, s: (0, 0, 0)),
            scratch_shapes=[
                pltpu.VMEM((seqs * tblock, cols), F32),
                pltpu.VMEM((seqs * tblock, kvcols), F32),
            ],
        ),
        compiler_params=pltpu.CompilerParams(vmem_limit_bytes=40 << 20),
    )(slot_seq, in_hbm(tokens), in_hbm(w_query), in_hbm(w_keyval_t))


def attend_kernel(slot, slot_seq, lengths, recv, keys_t, values, out, kn, vn, s_even, s_odd, top_even, top_odd):
    z = pl.program_id(0)
    last = pl.num_programs(0) - 1
    groups, shards, tblock, width = recv.shape
    new = groups * tblock
    cols = 2 * HD
    part = width - cols
    prefix = keys_t.shape[1]
    live = lengths[slot_seq[slot[0]]]
    factor = F32(1.4426950408889634 / 16.0)

    def score(plane, j, s_ref, top_ref):
        seen = lax.broadcasted_iota(jnp.int32, (1, prefix), 1) < live
        row = lax.broadcasted_iota(jnp.int32, (new, new), 0)
        causal = lax.broadcasted_iota(jnp.int32, (new, new), 1) <= row
        causal = jnp.concatenate([causal, causal], axis=0)
        at = j * HD
        qa = recv[:, 2 * plane, :, at : at + HD].reshape(new, HD)
        qb = recv[:, 2 * plane + 1, :, at : at + HD].reshape(new, HD)
        q = jnp.concatenate([qa, qb], axis=0)
        s = jnp.dot(q, keys_t[...], preferred_element_type=F32)
        sn = jnp.dot(q, kn[...], preferred_element_type=F32)
        s = jnp.where(seen, s, F32(NEG))
        sn = jnp.where(causal, sn, F32(NEG))
        s_ref[:, :prefix] = s
        s_ref[:, prefix:] = sn
        top = jnp.maximum(jnp.max(s, axis=1, keepdims=True), jnp.max(sn, axis=1, keepdims=True))
        top_ref[...] = jnp.broadcast_to(top, top_ref.shape)

    def weigh(j, s_ref, top_ref):
        low = lax.broadcasted_iota(jnp.int32, (1, tblock, 1), 1) < tblock // 2
        e = jnp.exp2((s_ref[...] - top_ref[:, :1]) * factor)
        scale = 1.0 / jnp.sum(e, axis=1, keepdims=True)
        p = (e * scale).astype(BF16)
        o = jnp.dot(p[:, :prefix], values[...], preferred_element_type=F32)
        o = o + jnp.dot(p[:, prefix:], vn[...], preferred_element_type=F32)
        a = o[:new].reshape(groups, tblock, HD)
        b = pltpu.roll(o[new:].reshape(groups, tblock, HD), tblock // 2, 1)
        at = j * HD
        out[:, 0, 0, :, at : at + HD] = jnp.where(low, a, b).astype(BF16)
        out[:, 0, 1, :, at : at + HD] = jnp.where(low, b, a).astype(BF16)

    @pl.when(z == 0)
    def _():
        each = HD // part
        pieces = [recv[:, h, :, cols:].reshape(new, part).astype(F32) for h in range(shards)]
        kn[...] = jnp.concatenate(pieces[:each], axis=1).T.astype(BF16)
        vn[...] = jnp.concatenate(pieces[each:], axis=1).astype(BF16)
        score(0, 0, s_even, top_even)

    score(z, 1, s_odd, top_odd)
    weigh(0, s_even, top_even)
    score(jnp.minimum(z + 1, last), 0, s_even, top_even)
    weigh(1, s_odd, top_odd)


def attend(slot, slot_seq, lengths, recv, keys_t, cache):
    groups, shards, tblock, width = recv.shape
    prefix = cache.shape[0]
    new = groups * tblock
    planes = shards // 2
    return pl.pallas_call(
        attend_kernel,
        name="attend",
        out_shape=jax.ShapeDtypeStruct((groups, planes, 2, tblock, 2 * HD), BF16),
        grid_spec=pltpu.PrefetchScalarGridSpec(
            num_scalar_prefetch=3,
            grid=(planes,),
            in_specs=[VMEM_WHOLE, VMEM_WHOLE, pl.BlockSpec((prefix, HD), lambda z, *_: (0, 1))],
            out_specs=pl.BlockSpec((groups, 1, 2, tblock, 2 * HD), lambda z, *_: (0, z, 0, 0, 0)),
            scratch_shapes=[
                pltpu.VMEM((HD, new), BF16),
                pltpu.VMEM((new, HD), BF16),
                pltpu.VMEM((2 * new, prefix + new), F32),
                pltpu.VMEM((2 * new, prefix + new), F32),
                pltpu.VMEM((2 * new, 128), F32),
                pltpu.VMEM((2 * new, 128), F32),
            ],
        ),
        compiler_params=pltpu.CompilerParams(vmem_limit_bytes=40 << 20),
    )(slot, slot_seq, lengths, recv, keys_t, cache)


def outproj_kernel(first, count, order, recv, w_own, w_other, *refs):
    outs, (own, other) = refs[:-2], refs[-2:]
    half = recv.shape[1] // 2

    low = lax.broadcasted_iota(jnp.int32, (2 * half, 1), 0) < half
    for i in range(0, count * 32, 4):
        mine, theirs = [], []
        for k in range(i, i + 4, 2):
            t0 = recv[order[first * 32 + k]].astype(F32)
            t1 = recv[order[first * 32 + k + 1]].astype(F32)
            mine.append(jnp.where(low, t0, pltpu.roll(t1, half, 0)))
            theirs.append(jnp.where(low, pltpu.roll(t0, half, 0), t1))
        rows = slice(i * half, (i + 4) * half)
        own[rows, :] = jnp.concatenate(mine, axis=0).astype(BF16)
        other[rows, :] = jnp.concatenate(theirs, axis=0).astype(BF16)

    rows = outs[0].shape[0]
    nblock = 512
    for n in range(0, w_own.shape[1], nblock):
        prod = jnp.dot(own[...], w_own[:, n : n + nblock], preferred_element_type=F32)
        prod = prod + jnp.dot(other[...], w_other[:, n : n + nblock], preferred_element_type=F32)
        prod = prod.astype(BF16)
        for i, out in enumerate(outs):
            out[:, n : n + nblock] = prod[i * rows : (i + 1) * rows]


def outproj(first, count, order, recv, w_own, w_other):
    depth, width = w_own.shape
    seqs, tblock, _ = recv.shape
    rows = 16 * (tblock // 2)
    return pl.pallas_call(
        lambda *refs: outproj_kernel(first, count, *refs),
        name="outproj%d" % first,
        out_shape=[jax.ShapeDtypeStruct((rows, width), BF16)] * (2 * count),
        in_specs=[pl.BlockSpec(memory_space=pltpu.SMEM), VMEM_WHOLE, VMEM_WHOLE, VMEM_WHOLE],
        out_specs=[VMEM_WHOLE] * (2 * count),
        scratch_shapes=[pltpu.VMEM((count * 2 * rows, depth), BF16)] * 2,
        compiler_params=pltpu.CompilerParams(vmem_limit_bytes=40 << 20),
    )(order, recv, w_own, w_other)


def shift(x, step, shards):
    planes = shards // 2
    perm = [(2 * z + c, 2 * ((z + step) % planes) + c) for z in range(planes) for c in range(2)]
    return lax.ppermute(x, "ha", perm)


def swap(x, shards):
    return lax.ppermute(x, "ha", [(h, h ^ 1) for h in range(shards)])


def on_device(tokens, w_query, w_keyval, w_out, cache_kv, lengths, slot_seq):
    seqs, tblock, width = tokens.shape
    groups = lax.axis_size("ba")
    shards = lax.axis_size("ha")
    ha = lax.axis_index("ha")
    plane, core = ha // 2, ha % 2

    w_other = swap(w_out, shards)
    sent = project(tokens, w_query, w_keyval.T, slot_seq)
    recv = lax.all_to_all(sent, ("ba", "ha"), split_axis=0, concat_axis=0, tiled=True)
    slot = (lax.axis_index("ba") * shards + ha).reshape(1)
    keys_t = cache_kv[0, :, :HD].T
    heads = attend(
        slot, slot_seq, lengths, recv.reshape(groups, shards, tblock, -1), keys_t, cache_kv[0]
    )
    back = lax.all_to_all(
        heads.reshape(seqs, tblock, 2 * HD), ("ba", "ha"), split_axis=0, concat_axis=0, tiled=True
    )

    slots = jnp.arange(seqs, dtype=jnp.int32)
    inverse = jnp.zeros((seqs,), jnp.int32).at[slot_seq].set(slots)
    chunk = (plane + jnp.array([2, 1, 3, 0], jnp.int32)) % (shards // 2)
    side = jnp.stack([1 - core, core])
    seq = (chunk[:, None, None] * 2 + side[None, :, None]) * 16 + jnp.arange(16, dtype=jnp.int32)
    order = jnp.take(inverse, seq.reshape(-1), axis=0)

    opp_a, opp_b = outproj(0, 1, order, back, w_out, w_other)
    from_a = shift(opp_a, 1, shards)
    from_b = shift(opp_b, -1, shards)
    up_a, up_b, down_a, down_b = outproj(1, 2, order, back, w_out, w_other)
    below_b = shift(up_b, 1, shards)
    above_a = shift(down_a, -1, shards)
    own_a, own_b = outproj(3, 1, order, back, w_out, w_other)
    below_a = shift((up_a.astype(F32) + from_a.astype(F32)).astype(BF16), 1, shards)
    above_b = shift((down_b.astype(F32) + from_b.astype(F32)).astype(BF16), -1, shards)

    give = (own_a.astype(F32) + below_a.astype(F32) + above_a.astype(F32)).astype(BF16)
    keep = (own_b.astype(F32) + below_b.astype(F32) + above_b.astype(F32)).astype(BF16)
    got = swap(give, shards)
    keep = keep.reshape(16, tblock // 2, width)
    got = got.reshape(16, tblock // 2, width)
    first = jnp.where(core == 0, keep, got)
    second = jnp.where(core == 0, got, keep)
    return jnp.concatenate([first, second], axis=1)


def solution(mesh):
    in_specs = (
        P(None, "ba", None),
        P(None, "ha"),
        P(None, "ha"),
        P("ha", None),
        P(("ba", "ha"), None, None),
        P(),
        P(),
    )
    out_specs = P("ha", "ba", None)
    return jax.shard_map(
        on_device, mesh=mesh, in_specs=in_specs, out_specs=out_specs, check_vma=False
    )
```
